32 devices in a mesh: seq: 16 (over z, y, x), img: 2 (over core).
Axes of the slice: x: 2, y: 2, z: 4, core: 2. Of those that a mesh axis runs over, the one named last changes fastest.
Arguments:
- inner_acts: bfloat16 [4096, 3072], P(('img', 'seq')), parts along dimension 0, may hold values from -6 to 6
- gate_acts: bfloat16 [4096, 3072], P(('img', 'seq')), parts along dimension 0, may hold values from -6 to 6
- state_proj: bfloat16 [4096, 64], P(('img', 'seq')), parts along dimension 0, may hold values from -3 to 3
- step_raw: bfloat16 [4096, 96], P(('img', 'seq')), parts along dimension 0, may hold values from -4 to 4
- conv_weight: float32 [2, 4, 3072], replicated, may hold values from -3 to 3
- conv_bias: float32 [2, 3072], replicated, may hold values from -3 to 3
- step_bias: float32 [2, 48], replicated, may hold values from -1.5 to 0.5
- decay_rate: float32 [2, 48], replicated, may hold values from 5e-06 to 0.04
- skip_gain: float32 [2, 48], replicated, may hold values from 0.5 to 2
- norm_gain: float32 [3072], replicated, may hold values from 0.5 to 1.5
Outputs:
- mixed: bfloat16 [4096, 3072], P(('img', 'seq')), parts along dimension 0
The draws below stay inside these ranges and needn't reach their ends.
There are 2 independent parts, one for each index of `img`. The reference program is written for one: setup_inputs(seed, part) draws one part's arguments, and reference() takes and returns one part's arrays. A program takes and returns all parts, laid end to end along the dimension named above; an argument that names none is the same for every part. Nothing has to cross between parts.
All inputs are finite; a program needn't handle non-finite values.
Results may differ from the reference program's by a relative error of at most 0.0058.
Values may be sent and summed in bfloat16 or wider, within the bound.
No kernel may reach another device: no remote copies, remote signals or barrier semaphores. Data moves between devices by JAX's collectives and lax.ppermute only.
A program may use at most 192 MiB of HBM per device.

```python
import math
import jax
import jax.numpy as jnp
from jax import lax

INNER = 3072
STATE = 16
KERNEL = 4
TOK_DEV = 128
HEADS = 48
TOKENS = 2048


def draw_step_raw(key, part):
    blocks = TOKENS // TOK_DEV
    offset_key = jax.random.fold_in(key, 11)
    noise_key = jax.random.fold_in(key, 12)
    offset = jax.random.uniform(offset_key, (blocks, 1, 2 * HEADS), jnp.float32, -3.0, 3.0)
    noise = jax.random.normal(noise_key, (blocks, TOK_DEV, 2 * HEADS), jnp.float32)
    values = jnp.clip(offset + noise, -4.0, 4.0)
    return values.reshape(TOKENS, 2 * HEADS).astype(jnp.bfloat16)


def shard_levels(rng, shape, split, low, high):
    level = 1.0
    for position, parts in split:
        draws = jax.random.uniform(jax.random.fold_in(jax.random.fold_in(rng, 6), position), (parts,), jnp.float32, low / len(split), high / len(split))
        level = level * jnp.repeat(jnp.exp(draws), shape[position] // parts).reshape((-1,) + (1,) * (len(shape) - 1 - position))
    return level


def gaussian(key, dims, deviation, limit, cuts=(), held_as=jnp.bfloat16):
    loudness = shard_levels(key, dims, cuts, -0.22, 0.18) if cuts else 1.0
    drawn = jax.random.normal(key, dims, jnp.float32) * deviation * loudness
    return jnp.minimum(jnp.maximum(drawn, -limit), limit).astype(held_as)


def setup_inputs(seed: int = 0, part: int = 0) -> dict:
    key_of = jax.random.split(jax.random.key(seed), 11)
    own_keys = jax.random.split(jax.random.fold_in(key_of[10], part), 11)
    return {
        "inner_acts": gaussian(own_keys[0], (TOKENS, INNER), 1.0, 6.0, ((0, 16),)),
        "gate_acts": gaussian(own_keys[1], (TOKENS, INNER), 1.0, 6.0, ((0, 16),)),
        "state_proj": gaussian(own_keys[2], (TOKENS, 4 * STATE), 0.5, 3.0, ((0, 16),)),
        "step_raw": draw_step_raw(jax.random.fold_in(jax.random.fold_in(key_of[10], part), 71), part),
        "conv_weight": gaussian(key_of[4], (2, KERNEL, INNER), 0.5, 3.0, (), jnp.float32),
        "conv_bias": gaussian(key_of[5], (2, INNER), 0.5, 3.0, (), jnp.float32),
        "step_bias": jnp.clip(jax.random.uniform(key_of[6], (2, HEADS), jnp.float32, -1.5, 0.5), -1.5, 0.5),
        "decay_rate": jnp.clip(jnp.exp(jax.random.uniform(key_of[7], (2, HEADS), jnp.float32, math.log(4.999999873689376e-06), math.log(0.04))), 4.999999873689376e-06, 0.04),
        "skip_gain": jnp.clip(jnp.exp(jax.random.uniform(key_of[8], (2, HEADS), jnp.float32, math.log(0.5), math.log(2.0))), 0.5, 2.0),
        "norm_gain": jnp.clip(1.0 + 0.1 * jax.random.normal(key_of[9], (INNER,), jnp.float32), 0.5, 1.5),
    }


def convolve(window, weight, bias):
    kernel = weight.shape[0]
    length = window.shape[0] - kernel + 1
    accum = jnp.zeros((length, window.shape[1]), jnp.float32) + bias[None, :]
    for offset in range(kernel):
        start = kernel - 1 - offset
        accum = accum + weight[offset][None, :] * window[start:start + length].astype(jnp.float32)
    return jax.nn.silu(accum).astype(jnp.bfloat16)

def block_terms(conved, write_rows, read_rows, raw_step, step_bias, rate, skip):
    length, width = conved.shape
    heads = raw_step.shape[1]
    step_size = jax.nn.softplus(raw_step.astype(jnp.float32) + step_bias[None, :])
    cumul = jnp.cumsum(-rate[None, :] * step_size, axis=0)
    later = lax.broadcasted_iota(jnp.int32, (length, length), 0)
    earlier = lax.broadcasted_iota(jnp.int32, (length, length), 1)
    causal = (later >= earlier)[None]
    spread = cumul.T[:, :, None] - cumul.T[:, None, :]
    decay = jnp.where(causal, jnp.exp(jnp.where(causal, spread, 0.0)), 0.0)
    scores = jnp.dot(read_rows, write_rows.T, preferred_element_type=jnp.float32)
    weights = (scores[None] * decay * step_size.T[:, None, :]).astype(jnp.bfloat16)
    per_head = conved.reshape(length, heads, width // heads)
    inside = jnp.einsum('hts,shp->thp', weights.astype(jnp.float32), per_head.astype(jnp.float32))
    final_log = cumul[-1]
    carried = jnp.exp(final_log[None, :] - cumul) * step_size
    loaded = (carried[:, :, None] * write_rows.astype(jnp.float32)[:, None, :]).astype(jnp.bfloat16)
    end_state = jnp.einsum('shp,shn->hpn', per_head.astype(jnp.float32), loaded.astype(jnp.float32))
    base = inside + skip[None, :, None] * per_head.astype(jnp.float32)
    return (base, cumul, jnp.exp(final_log), end_state)

def inter_terms(cumul, read_rows, incoming):
    readout = jnp.einsum('tn,hpn->thp', read_rows.astype(jnp.float32), incoming, precision=lax.Precision.HIGHEST)
    return readout * jnp.exp(cumul)[:, :, None]

def direction(acts, write_rows, read_rows, raw_step, weight, bias, step_bias, rate, skip):
    kernel = weight.shape[0]
    width = acts.shape[1]
    heads = raw_step.shape[1]
    window = jnp.concatenate([jnp.zeros((kernel - 1, width), acts.dtype), acts], axis=0)
    conved = convolve(window, weight, bias)
    blocks = conved.shape[0] // TOK_DEV
    pieces = (conved.reshape(blocks, TOK_DEV, width), write_rows.reshape(blocks, TOK_DEV, -1), read_rows.reshape(blocks, TOK_DEV, -1), raw_step.reshape(blocks, TOK_DEV, heads))

    def advance(incoming, piece):
        conved_block, write_block, read_block, raw_block = piece
        base, cumul, total, end_state = block_terms(conved_block, write_block, read_block, raw_block, step_bias, rate, skip)
        result = (base + inter_terms(cumul, read_block, incoming)).reshape(TOK_DEV, width)
        return (total[:, None, None] * incoming + end_state, result)
    initial = jnp.zeros((heads, width // heads, write_rows.shape[1]), jnp.float32)
    final_state, outputs = lax.scan(advance, initial, pieces)
    return outputs.reshape(-1, width)

def reference(inner_acts, gate_acts, state_proj, step_raw, conv_weight, conv_bias, step_bias, decay_rate, skip_gain, norm_gain):
    forward = direction(inner_acts, state_proj[:, 0:STATE], state_proj[:, STATE:2 * STATE], step_raw[:, :HEADS], conv_weight[0], conv_bias[0], step_bias[0], decay_rate[0], skip_gain[0])
    flipped_proj = state_proj[::-1]
    backward = direction(inner_acts[::-1], flipped_proj[:, 2 * STATE:3 * STATE], flipped_proj[:, 3 * STATE:4 * STATE], step_raw[::-1][:, HEADS:], conv_weight[1], conv_bias[1], step_bias[1], decay_rate[1], skip_gain[1])[::-1]
    gated = (forward + backward) * jax.nn.silu(gate_acts.astype(jnp.float32))
    scale = lax.rsqrt(lax.optimization_barrier(jnp.mean(gated * gated, axis=1, keepdims=True)) + 1e-05)
    return (gated * scale * norm_gain[None, :]).astype(jnp.bfloat16)
```

```python
import functools
import jax
import jax.numpy as jnp
from jax import lax
from jax.experimental import pallas as pl
from jax.experimental.pallas import tpu as pltpu
from jax.sharding import PartitionSpec as P

F32, BF16 = jnp.float32, jnp.bfloat16
LANES = 128
SUB = 8


def partner(me, k, count):
    if count & (count - 1) == 0:
        return me ^ k, me ^ k
    return lax.rem(me - k + count, count), lax.rem(me + k, count)


def pairs(k, count, stride, total):
    out = []
    for i in range(total):
        pos = (i // stride) % count
        dest = pos ^ k if count & (count - 1) == 0 else (pos + k) % count
        out.append((i, i + (dest - pos) * stride))
    return out


def silu(v):
    h = 0.5 * v
    return h + h * jnp.tanh(h)


def softplus(v):
    return jnp.maximum(v, 0.0) + jnp.log1p(jnp.exp(-jnp.abs(v)))


def split(v, parts):
    out = []
    for _ in range(parts):
        top = v.astype(BF16)
        out.append(top)
        v = v - top.astype(F32)
    return out


def dot(a, b, dims=(((1,), (0,)), ((), ()))):
    return lax.dot_general(a, b, dims, preferred_element_type=F32)


def rows_of(shape):
    return lax.broadcasted_iota(jnp.int32, shape, 0)


def lanes_of(shape):
    return lax.broadcasted_iota(jnp.int32, shape, 1)


def spread(rows, repeat, head, start, width):
    r, c = rows_of((rows, width)), lanes_of((rows, width)) + start
    if repeat < rows:
        r = jnp.where(r >= repeat, r - repeat, r)
    first = r * head
    return jnp.where((c >= first) & (c < first + head), 1.0, 0.0).astype(BF16)


def doubled(v):
    return jnp.concatenate(split(v, 2), axis=1)


def scan_parts(d, raw_ref, bias_ref, rate_ref):
    heads = raw_ref.shape[1] // 2
    length = raw_ref.shape[0]
    raw = raw_ref[:, d * heads : (d + 1) * heads].astype(F32)
    step = softplus(raw + bias_ref[d : d + 1, :])
    t, s = rows_of((length, length)), lanes_of((length, length))
    tri = jnp.where(s <= t if d == 0 else s >= t, 1.0, 0.0)
    cumul = jnp.dot(
        tri, -rate_ref[d : d + 1, :] * step, precision=lax.Precision.HIGHEST,
        preferred_element_type=F32,
    )
    return step, cumul


def projections(d, proj_ref):
    state = proj_ref.shape[1] // 4
    write = proj_ref[:, 2 * d * state : (2 * d + 1) * state]
    read = proj_ref[:, (2 * d + 1) * state : (2 * d + 2) * state]
    return write, read


def conv_rows(d, x, cw_ref, cb_ref, lanes):
    length = x.shape[0]
    taps = cw_ref.shape[1]
    acc = cb_ref[d : d + 1, lanes] + cw_ref[d, 0:1, lanes] * x
    for k in range(1, taps):
        moved = pltpu.roll(x, k if d == 0 else length - k, 0)
        acc = acc + cw_ref[d, k : k + 1, lanes] * moved
    return silu(acc).astype(BF16)


def edge_conv(d, window, cw_ref, cb_ref, lanes):
    taps = cw_ref.shape[1]
    acc = cb_ref[d : d + 1, lanes]
    for k in range(taps):
        shift = taps - 1 - k if d == 0 else k
        moved = window if shift == 0 else pltpu.roll(window, SUB - shift, 0)
        acc = acc + cw_ref[d, k : k + 1, lanes] * moved
    return silu(acc).astype(BF16)


def edge_mask(d, length, taps):
    t = rows_of((length, 1))
    return t >= taps - 1 if d == 0 else t < length - (taps - 1)


def coef_rows(blocks, per_row):
    return -(-blocks // per_row)


def place(tile, coefs, per_row, block, first_row):
    row = rows_of(tile.shape)
    for j in range(SUB - first_row):
        index = j * per_row + block
        if index < len(coefs):
            tile = jnp.where(row == first_row + j, coefs[index], tile)
    return tile


def fetch(tile, index, per_row, first_row):
    j, block = divmod(index, per_row)
    return tile[first_row + j : first_row + j + 1, block * LANES : (block + 1) * LANES]


def stacked(rows):
    row = rows_of((SUB, rows[0].shape[1]))
    out = jnp.zeros((SUB, rows[0].shape[1]), F32)
    for j, value in enumerate(rows):
        out = jnp.where(row == j, value, out)
    return out


def widen(v):
    pad = LANES - v.shape[1]
    return jnp.concatenate([v, jnp.zeros((v.shape[0], pad), F32)], axis=1)


def ends_kernel(dims, x_ref, proj_ref, raw_ref, cw_ref, cb_ref, bias_ref, rate_ref, *outs):
    group, head, chunk, axis = dims
    length, width = x_ref.shape
    heads = raw_ref.shape[1] // 2
    taps = cw_ref.shape[1]
    state = proj_ref.shape[1] // 4
    edge = taps - 1
    part = width // group
    per_row = part // LANES
    me = lax.rem(lax.axis_index(axis), group)
    carried, writes, coefs, logs = [], [], [], []
    for d in range(2):
        step, cumul = scan_parts(d, raw_ref, bias_ref, rate_ref)
        last = cumul[length - 1 : length] if d == 0 else cumul[0:1]
        weight = jnp.exp(last - cumul) * step
        carried.append(doubled(jnp.where(edge_mask(d, length, taps), weight, 0.0)))
        write = projections(d, proj_ref)[0]
        writes.append(write)
        for j in range(edge):
            r = j if d == 0 else length - edge + j
            coefs.append(
                widen(
                    jnp.concatenate([weight[r : r + 1], write.astype(F32)[r : r + 1]], axis=1)
                )
            )
        logs += [widen(p.astype(F32)) for p in split(last, 3)]
    coefs = coefs + logs
    for k in range(group):
        out_ref = outs[k]
        target = partner(me, k, group)[1]
        for j in range(part // chunk):
            start = pl.multiple_of(target * part + j * chunk, chunk)
            lanes = pl.ds(start, chunk)
            here = slice(j * chunk, (j + 1) * chunk)
            x = x_ref[:, lanes].astype(F32)
            match = spread(2 * heads, heads, head, start, chunk)
            for d in range(2):
                conved = conv_rows(d, x, cw_ref, cb_ref, lanes)
                loaded = (conved.astype(F32) * dot(carried[d], match)).astype(BF16)
                end = dot(writes[d], loaded, (((0,), (0,)), ((), ())))
                out_ref[d * state : (d + 1) * state, here] = end.astype(BF16)
            row = rows_of((SUB, chunk))
            tail = pltpu.roll(x[length - SUB :], SUB - (SUB - 2 * edge), 0)
            tile = jnp.where(row < edge, x[:SUB], jnp.where(row < 2 * edge, tail, 0.0))
            for i in range(chunk // LANES):
                block = j * (chunk // LANES) + i
                piece = place(
                    tile[:, i * LANES : (i + 1) * LANES], coefs, per_row, block, 2 * edge
                )
                out_ref[2 * state :, block * LANES : (block + 1) * LANES] = piece.astype(BF16)


def inside_kernel(
    dims, x_ref, proj_ref, raw_ref, cw_ref, cb_ref, bias_ref, rate_ref, skip_ref, y_ref
):
    group, head, chunk, axis = dims
    length, width = x_ref.shape
    heads = raw_ref.shape[1] // 2
    taps = cw_ref.shape[1]
    t, s = rows_of((length, length)), lanes_of((length, length))
    before, after, mixes, skips, masks = [], [], [], [], []
    for d in range(2):
        step, cumul = scan_parts(d, raw_ref, bias_ref, rate_ref)
        mask = edge_mask(d, length, taps)
        before.append(doubled(jnp.where(mask, jnp.exp(-cumul) * step, 0.0)))
        after.append(doubled(jnp.exp(cumul)))
        write, read = projections(d, proj_ref)
        scores = dot(read, write, (((1,), (1,)), ((), ())))
        mixes.append(jnp.where(s <= t if d == 0 else s >= t, scores, 0.0).astype(BF16))
        skips.append(doubled(skip_ref[d : d + 1, :]))
        masks.append(mask)
    for j in range(width // chunk):
        lanes = slice(j * chunk, (j + 1) * chunk)
        x = x_ref[:, lanes].astype(F32)
        match = spread(2 * heads, heads, head, j * chunk, chunk)
        total = None
        for d in range(2):
            conved = conv_rows(d, x, cw_ref, cb_ref, lanes).astype(F32)
            scaled = (conved * dot(before[d], match)).astype(BF16)
            inner = dot(mixes[d], scaled) * dot(after[d], match)
            direct = jnp.where(masks[d], conved * dot(skips[d], match), 0.0)
            total = inner + direct if total is None else total + inner + direct
        y_ref[:, lanes] = total


def expand_rows(tiles, head, start, width):
    match = spread(LANES, LANES, head, start, width)
    wide = dot(jnp.concatenate(tiles, axis=0).astype(BF16), match)
    return [wide[i * SUB : (i + 1) * SUB] for i in range(len(tiles))]


def edge_state(d, window, wide, coef, heads, state, edge, cw_ref, cb_ref, lanes):
    conved = edge_conv(d, window, cw_ref, cb_ref, lanes).astype(F32)
    row = rows_of(window.shape)
    value = jnp.where(row < edge, conved * wide, 0.0).astype(BF16)
    write = coef[:, heads : heads + state]
    write = jnp.where(rows_of(write.shape) < edge, write, 0.0).astype(BF16)
    return dot(write, value, (((0,), (0,)), ((), ())))


def window_of(d, before, here, after, edge):
    row = rows_of(here.shape)
    up, down = SUB - edge, edge
    if d == 0:
        return jnp.where(row < edge, pltpu.roll(before, up, 0), pltpu.roll(here, down, 0))
    return jnp.where(row < edge, pltpu.roll(here, up, 0), pltpu.roll(after, down, 0))


def group_kernel(dims, cw_ref, cb_ref, *refs):
    group, count, head, heads, state, edge, axis = dims
    ins, refs = refs[:group], refs[group:]
    outs, refs = refs[: count - 1], refs[count - 1 :]
    own_ref, kept_ref, tiles_ref, wide_ref, slots = refs
    part = ins[0].shape[1]
    per_row = part // LANES
    place_in = lax.axis_index(axis)
    me, mine = lax.rem(place_in, group), lax.div(place_in, group)
    start = pl.multiple_of(me * part, LANES)
    lanes = pl.ds(start, part)
    for k in range(group):
        slots[partner(me, k, group)[0]] = ins[k][...]
    tiles = [slots[p, 2 * state :, :].astype(F32) for p in range(group)]
    row128 = rows_of((SUB, LANES))
    small, log_of = [], []
    for p in range(group):
        for d in range(2):
            base = d * edge
            rows = [fetch(tiles[p], base + j, per_row, 2 * edge) for j in range(edge)]
            at = 2 * edge + 3 * d
            log = sum(fetch(tiles[p], at + j, per_row, 2 * edge) for j in range(3))
            log_of.append(log)
            parts = [v.astype(F32) for v in split(jnp.exp(log), 2)]
            small.append(stacked(rows + parts))
    wide = expand_rows(small, head, start, part)
    zero = jnp.zeros((state, part), F32)
    totals, ends = [], []
    for d in range(2):
        order = range(group) if d == 0 else range(group - 1, -1, -1)
        running = zero
        for p in order:
            w = wide[2 * p + d]
            total = w[edge : edge + 1] + w[edge + 1 : edge + 2]
            kept = slots[p, d * state : (d + 1) * state, :].astype(F32)
            if p != order[0]:
                window = window_of(
                    d, tiles[p - 1] if d == 0 else None, tiles[p],
                    tiles[p + 1] if d == 1 else None, edge,
                )
                kept = kept + edge_state(
                    d, window, w, small[2 * p + d], heads, state, edge, cw_ref, cb_ref, lanes
                )
            kept_ref[d, p] = kept
            running = total * running + kept
            wide_ref[d, p] = w
        ends.append(running)
    for p in range(group):
        tiles_ref[p] = tiles[p]
    lane = lanes_of((SUB, LANES))
    row = rows_of((SUB, part))
    edges = jnp.where(row < edge, tiles[0], tiles[group - 1])
    messages = []
    for d in range(2):
        bound = 0 if d == 0 else group - 1
        others = [p for p in range(group) if p != bound]
        sum_log = log_of[2 * bound + d] * 0.0
        for p in others:
            sum_log = sum_log + log_of[2 * p + d]
        scale = jnp.where(lane < heads, jnp.exp(sum_log), 1.0)
        all_log = sum_log + log_of[2 * bound + d]
        sent = small[2 * bound + d] * scale
        logs = [v.astype(F32) for v in split(all_log, 3)]
        pieces, mine_pieces = [], []
        for i in range(per_row):
            cut = edges[:, i * LANES : (i + 1) * LANES]
            far = [sent[j : j + 1] for j in range(edge)] + logs
            near = [small[2 * bound + d][j : j + 1] for j in range(edge)] + logs
            clean = jnp.where(row128 < 2 * edge, cut, 0.0)
            pieces.append(place(clean, far, per_row, i, 2 * edge))
            mine_pieces.append(place(clean, near, per_row, i, 2 * edge))
        messages.append(jnp.concatenate(pieces, axis=1))
        own_ref[d] = jnp.concatenate(mine_pieces, axis=1)
    for k in range(1, count):
        forward = partner(mine, k, count)[1] > mine
        out_ref = outs[k - 1]
        out_ref[:state, :] = jnp.where(forward, ends[0], ends[1]).astype(BF16)
        out_ref[state:, :] = jnp.where(forward, messages[0], messages[1]).astype(BF16)


def enter_kernel(dims, cw_ref, cb_ref, *refs):
    group, count, head, heads, state, edge, axis = dims
    ins, refs = refs[: count - 1], refs[count - 1 :]
    (own_ref, kept_ref, tiles_ref, wide_ref), refs = refs[:4], refs[4:]
    outs, refs = refs[:group], refs[group:]
    far_ref, near_ref, slots = refs
    part = own_ref.shape[2]
    per_row = part // LANES
    place_in = lax.axis_index(axis)
    me, mine = lax.rem(place_in, group), lax.div(place_in, group)
    start = pl.multiple_of(me * part, LANES)
    lanes = pl.ds(start, part)
    for k in range(1, count):
        source = partner(mine, k, count)[0]
        far_ref[source] = ins[k - 1][:state, :].astype(F32)
        tile = ins[k - 1][state:, :].astype(F32)
        near_ref[0, source] = tile
        near_ref[1, source] = tile
    far_ref[mine] = jnp.zeros((state, part), F32)
    near_ref[0, mine] = own_ref[0]
    near_ref[1, mine] = own_ref[1]
    small = []
    for p in range(count):
        for d in range(2):
            tile = near_ref[d, p]
            rows = [fetch(tile, j, per_row, 2 * edge) for j in range(edge)]
            log = sum(fetch(tile, edge + j, per_row, 2 * edge) for j in range(3))
            parts = [v.astype(F32) for v in split(jnp.exp(log), 2)]
            small.append(stacked(rows + parts))
    wide = expand_rows(small, head, start, part)
    nothing = jnp.zeros((SUB, part), F32)
    row = rows_of((SUB, part))
    coming, bounds = [], []
    for d in range(2):
        order = range(count) if d == 0 else range(count - 1, -1, -1)
        running = jnp.zeros((state, part), F32)
        bound = jnp.zeros((state, part), F32)
        for p in order:
            w = wide[2 * p + d]
            before = near_ref[0, p - 1] if p > 0 else nothing
            after = near_ref[1, p + 1] if p < count - 1 else nothing
            window = window_of(d, before, near_ref[d, p], after, edge)
            added = edge_state(
                d, window, w, small[2 * p + d], heads, state, edge, cw_ref, cb_ref, lanes
            )
            total = w[edge : edge + 1] + w[edge + 1 : edge + 2]
            longer = total * running + (far_ref[p] + added)
            earlier = p < mine if d == 0 else p > mine
            running = jnp.where(earlier, longer, running)
            bound = jnp.where(mine == p, added, bound)
        coming.append(running)
        bounds.append(bound)
    for d in range(2):
        order = range(group) if d == 0 else range(group - 1, -1, -1)
        running = coming[d]
        for p in order:
            slots[p, d * state : (d + 1) * state, :] = running.astype(BF16)
            w = wide_ref[d, p]
            total = w[edge : edge + 1] + w[edge + 1 : edge + 2]
            kept = kept_ref[d, p]
            if p == order[0]:
                kept = kept + bounds[d]
            running = total * running + kept
    outer_before = jnp.where(mine > 0, near_ref[0, jnp.maximum(mine - 1, 0)], 0.0)
    outer_after = jnp.where(mine < count - 1, near_ref[1, jnp.minimum(mine + 1, count - 1)], 0.0)
    for p in range(group):
        before = tiles_ref[p - 1] if p > 0 else outer_before
        after = tiles_ref[p + 1] if p < group - 1 else outer_after
        halo = jnp.where(
            row < edge, pltpu.roll(before, SUB - edge, 0),
            jnp.where(row < 2 * edge, pltpu.roll(after, edge, 0), 0.0),
        )
        slots[p, 2 * state :, :] = halo.astype(BF16)
    for k in range(group):
        outs[k][...] = slots[partner(me, k, group)[1]]


def finish_kernel(
    dims, y_ref, gate_ref, x_ref, proj_ref, raw_ref, cw_ref, cb_ref, bias_ref, rate_ref,
    skip_ref, gain_ref, *refs
):
    group, head, chunk, axis = dims
    ins, (out_ref, held) = refs[:group], refs[group:]
    length, width = x_ref.shape
    heads = raw_ref.shape[1] // 2
    taps = cw_ref.shape[1]
    edge = taps - 1
    state = proj_ref.shape[1] // 4
    part = width // group
    me = lax.rem(lax.axis_index(axis), group)
    t, s = rows_of((length, SUB)), lanes_of((length, SUB))
    reads, after, before, skips = [], [], [], []
    for d in range(2):
        step, cumul = scan_parts(d, raw_ref, bias_ref, rate_ref)
        after.append(doubled(jnp.exp(cumul)))
        u = jnp.exp(-cumul) * step
        write, read = projections(d, proj_ref)
        write = write.astype(F32)
        if d == 0:
            u, write = u[:SUB], write[:SUB]
            allowed = (s <= t) & (s < edge)
        else:
            u = pltpu.roll(u[length - SUB :], edge, 0)
            write = pltpu.roll(write[length - SUB :], edge, 0)
            allowed = (s + length - edge >= t) & (s < edge)
        u = jnp.where(rows_of(u.shape) < edge, u, 0.0)
        before.append(doubled(u))
        scores = dot(read, write.astype(BF16), (((1,), (1,)), ((), ())))
        scores = jnp.where(allowed, scores, 0.0)
        reads.append(jnp.concatenate([read.astype(F32), scores], axis=1).astype(BF16))
        skips.append(doubled(skip_ref[d : d + 1, :]))
    squares = jnp.zeros((length, 1), F32)
    row = rows_of((SUB, chunk))
    for k in range(group):
        source = partner(me, k, group)[0]
        for j in range(part // chunk):
            start = pl.multiple_of(source * part + j * chunk, chunk)
            lanes = pl.ds(start, chunk)
            here = slice(j * chunk, (j + 1) * chunk)
            match = spread(2 * heads, heads, head, start, chunk)
            halo = ins[k][2 * state :, here].astype(F32)
            total = y_ref[:, lanes]
            for d in range(2):
                if d == 0:
                    near = x_ref[: 2 * SUB, lanes].astype(F32)[:SUB]
                    window = jnp.where(row < edge, halo, pltpu.roll(near, edge, 0))
                else:
                    near = x_ref[length - 2 * SUB :, lanes].astype(F32)[SUB:]
                    window = jnp.where(row < edge, pltpu.roll(near, edge, 0), halo)
                conved = edge_conv(d, window, cw_ref, cb_ref, lanes).astype(F32)
                conved = jnp.where(row < edge, conved, 0.0)
                scaled = conved * dot(before[d], match)
                coming = ins[k][d * state : (d + 1) * state, here].astype(F32)
                right = jnp.concatenate([coming, scaled], axis=0).astype(BF16)
                added = dot(reads[d], right) * dot(after[d], match)
                direct = conved * dot(skips[d], match)
                if d == 0:
                    direct = jnp.concatenate(
                        [direct, jnp.zeros((length - SUB, chunk), F32)], axis=0
                    )
                else:
                    direct = jnp.concatenate(
                        [jnp.zeros((length - SUB, chunk), F32), pltpu.roll(direct, SUB - edge, 0)],
                        axis=0,
                    )
                total = total + added + direct
            gated = total * silu(gate_ref[:, lanes].astype(F32))
            held[:, lanes] = gated
            squares = squares + jnp.sum(gated * gated, axis=1, keepdims=True)
    scale = lax.rsqrt(squares / width + 1e-05)
    for j in range(width // chunk):
        lanes = slice(j * chunk, (j + 1) * chunk)
        out_ref[:, lanes] = (held[:, lanes] * scale * gain_ref[:, lanes]).astype(BF16)


def call(body, outs, args, scratch=(), flops=0, name=None):
    vmem = pl.BlockSpec(memory_space=pltpu.VMEM)
    return pl.pallas_call(
        body,
        out_shape=outs,
        in_specs=[vmem] * len(args),
        out_specs=jax.tree.map(lambda _: vmem, outs),
        scratch_shapes=list(scratch),
        cost_estimate=pl.CostEstimate(flops=flops, bytes_accessed=1 << 20, transcendentals=0),
        name=name,
    )(*args)


def local(
    axis, ranks, inner_acts, gate_acts, state_proj, step_raw, conv_weight, conv_bias, step_bias,
    decay_rate, skip_gain, norm_gain,
):
    length, width = inner_acts.shape
    heads = step_raw.shape[1] // 2
    head = width // heads
    state = state_proj.shape[1] // 4
    edge = conv_weight.shape[1] - 1
    group = 1
    for g in range(1, ranks + 1):
        fits = width % (g * LANES) == 0 and (
            2 * edge + coef_rows(2 * edge + 6, width // (g * LANES)) <= SUB
        )
        if ranks % g == 0 and g * g <= ranks and fits:
            group = g
    count = ranks // group
    part = width // group
    chunk = 2 * LANES if part % (2 * LANES) == 0 else LANES
    tile_rows = SUB
    shape = jax.ShapeDtypeStruct
    dims = (group, head, chunk, axis)
    params = (conv_weight, conv_bias, step_bias, decay_rate)
    tokens = (inner_acts, state_proj, step_raw)
    big = length * width
    message = shape((2 * state + tile_rows, part), BF16)
    ends = call(
        functools.partial(ends_kernel, dims), [message] * group, tokens + params,
        flops=big * 400, name="ends",
    )
    got = [ends[0]] + [
        lax.ppermute(ends[k], axis, pairs(k, group, 1, ranks)) for k in range(1, group)
    ]
    inside = call(
        functools.partial(inside_kernel, dims), shape((length, width), F32),
        tokens + params + (skip_gain,), flops=big * 800, name="inside",
    )
    wide_dims = (group, count, head, heads, state, edge, axis)
    outs = call(
        functools.partial(group_kernel, wide_dims),
        [shape((state + tile_rows, part), BF16)] * (count - 1)
        + [
            shape((2, tile_rows, part), F32),
            shape((2, group, state, part), F32),
            shape((group, tile_rows, part), F32),
            shape((2, group, tile_rows, part), F32),
        ],
        (conv_weight, conv_bias, *got),
        scratch=[pltpu.VMEM((group, 2 * state + tile_rows, part), BF16)],
        flops=big * 100, name="group",
    )
    sent, rest = outs[: count - 1], outs[count - 1 :]
    far = [
        lax.ppermute(sent[k - 1], axis, pairs(k, count, group, ranks)) for k in range(1, count)
    ]
    enter = call(
        functools.partial(enter_kernel, wide_dims), [message] * group,
        (conv_weight, conv_bias, *far, *rest),
        scratch=[
            pltpu.VMEM((count, state, part), F32),
            pltpu.VMEM((2, count, tile_rows, part), F32),
            pltpu.VMEM((group, 2 * state + tile_rows, part), BF16),
        ],
        flops=big * 100, name="enter",
    )
    back = [enter[0]] + [
        lax.ppermute(enter[k], axis, pairs(k, group, 1, ranks)) for k in range(1, group)
    ]
    return call(
        functools.partial(finish_kernel, dims), shape((length, width), BF16),
        (inside, gate_acts, *tokens, *params, skip_gain, norm_gain[None, :], *back),
        scratch=[pltpu.VMEM((length, width), F32)], flops=big * 800, name="finish",
    )


def solution(mesh):
    axis = "seq"
    rows = P(("img", axis), None)
    return jax.shard_map(
        functools.partial(local, axis, mesh.shape[axis]),
        mesh=mesh,
        in_specs=(rows,) * 4 + (P(),) * 6,
        out_specs=rows,
        check_vma=False,
    )
```
